32 devices in a mesh: dp: 2 (over x), tp: 16 (over y, z, core).
Axes of the slice: x: 2, y: 2, z: 4, core: 2. Of those that a mesh axis runs over, the one named last changes fastest.
Arguments:
- x: bfloat16 [4096, 4096], P('dp'), parts along dimension 0
- dy: bfloat16 [4096, 4096], P('dp'), parts along dimension 0
- gate: bfloat16 [4096, 12288], P('dp', 'tp'), parts along dimension 0
- up: bfloat16 [4096, 12288], P('dp', 'tp'), parts along dimension 0
- w_gate: bfloat16 [4096, 12288], P(None, 'tp')
- w_up: bfloat16 [4096, 12288], P(None, 'tp')
- w_down: bfloat16 [12288, 4096], P('tp')
Outputs:
- output 1: bfloat16 [4096, 4096], P('dp'), parts along dimension 0
- output 2: bfloat16 [8192, 12288], P('dp', 'tp'), parts along dimension 0
- output 3: bfloat16 [8192, 12288], P('dp', 'tp'), parts along dimension 0
- output 4: bfloat16 [24576, 4096], P(('dp', 'tp')), parts along dimension 0
There are 2 independent parts. The reference program is written for one: setup_inputs(seed, part) draws one part's arguments, and reference() takes and returns one part's arrays. A program takes and returns all parts, laid end to end along the dimension named above; an argument that names none is the same for every part.
All inputs are finite; a program needn't handle non-finite values.
Results may differ from the reference program's by a relative error of at most 0.012.
Values are sent between devices in bfloat16 or wider.
A program may use at most 2 GiB of HBM per device.

```python
import jax
import jax.numpy as jnp

ROWS = 2048
D = 4096
FF = 12288


def act(gate, up):
    return jax.nn.silu(gate) * up


def setup_inputs(seed: int = 0, part: int = 0) -> dict:
    kx, ky, ka, kb, kg, ku, kd = jax.random.split(jax.random.key(seed), 7)
    kx, ky, ka, kb = (jax.random.fold_in(k, part) for k in (kx, ky, ka, kb))
    drawn = {
        "x": jax.random.normal(kx, (ROWS, D), jnp.float32),
        "dy": jax.random.normal(ky, (ROWS, D), jnp.float32),
        "gate": jax.random.normal(ka, (ROWS, FF), jnp.float32),
        "up": jax.random.normal(kb, (ROWS, FF), jnp.float32),
        "w_gate": jax.random.normal(kg, (D, FF), jnp.float32) * D**-0.5,
        "w_up": jax.random.normal(ku, (D, FF), jnp.float32) * D**-0.5,
        "w_down": jax.random.normal(kd, (FF, D), jnp.float32) * FF**-0.5,
    }
    return {k: v.astype(jnp.bfloat16) for k, v in drawn.items()}


def reference(x, dy, gate, up, w_gate, w_up, w_down):
    hidden, back = jax.vjp(act, gate.astype(jnp.float32), up.astype(jnp.float32))
    d_hidden = jnp.dot(dy, w_down.T, preferred_element_type=jnp.float32)
    d_gate, d_up = (g.astype(jnp.bfloat16) for g in back(d_hidden))
    dx = jnp.dot(d_gate, w_gate.T, preferred_element_type=jnp.float32) + jnp.dot(d_up, w_up.T, preferred_element_type=jnp.float32)
    dw_gate = jnp.dot(x.T, d_gate, preferred_element_type=jnp.float32)
    dw_up = jnp.dot(x.T, d_up, preferred_element_type=jnp.float32)
    dw_down = jnp.dot(hidden.astype(jnp.bfloat16).T, dy, preferred_element_type=jnp.float32)
    return tuple(g.astype(jnp.bfloat16) for g in (dx, dw_gate, dw_up, dw_down))
```

```python
import jax
import jax.numpy as jnp
from jax import lax
from jax.experimental import pallas as pl
from jax.experimental.pallas import tpu as pltpu
from jax.sharding import PartitionSpec as P

F32, BF16 = jnp.float32, jnp.bfloat16
ROWS, D, F = 2048, 4096, 768
BR = 512
BC = 512
NG = 2048 // BC
N = (ROWS // BR) * NG
H = BC // 2
OFF = (0, 1, 3, 5, 7, 9, 11, 13, 15, 17)
NA = OFF[5] + 1
DW0 = 17
TW = 256
NW = D // TW
T = max(N + OFF[9], DW0 + NW)
DEPTH = 4
NT = (((1,), (1,)), ((), ()))
TN = (((0,), (0,)), ((), ()))


def mm(a, b, dims):
    return lax.dot_general(a, b, dims, preferred_element_type=F32)


def ds(start, size):
    return pl.ds(pl.multiple_of(start, size), size)


class Chan:
    def __init__(self, cond, src, dst, send, recv=None, dev=None, depth=DEPTH):
        self.cond, self.src, self.dst, self.send, self.recv, self.dev, self.depth = cond, src, dst, send, recv, dev, depth

    def desc(self, k):
        sem = self.send.at[lax.rem(k, self.depth)]
        if self.dev is None:
            return pltpu.make_async_copy(self.src(k), self.dst(k), sem)
        return pltpu.make_async_remote_copy(
            self.src(k), self.dst(k), sem, self.recv(k), device_id=self.dev, device_id_type=pl.DeviceIdType.MESH
        )

    def _wait(self, k):
        if self.dev is None:
            self.desc(k).wait()
        else:
            self.desc(k).wait_send()

    def ready(self, k):
        @pl.when(k >= self.depth)
        def _():
            self._wait(k - self.depth)

    def start(self, k):
        self.desc(k).start()

    def go(self, k):
        self.ready(k)
        self.start(k)

    def drain(self, n):
        def run():
            @pl.loop(n - self.depth, n)
            def _(k):
                self._wait(k)

        if self.cond is None:
            run()
        else:
            pl.when(self.cond)(run)


def kernel(x, dy, gate, up, wg_h, wu_h, wd_h, out, dwg, dwu, dwd,
           wd, wg, wu, dgu, hT, dyb, gb, ub, d2d_st, d2d_rv, tmp, accA, accB,
           yA_rv, zA_rv, zB_rv, yB_rv, yA_st, zA_st, zB_st, yB_st, fA_st, fB_st, o_gu, o_d,
           ld, tl, ss, rs, d2d_r, credit):
    tp = lax.axis_index("tp")
    y, z, c = tp // 8, lax.rem(tp // 2, 4), lax.rem(tp, 2)

    def dev(yy, zz, cc):
        return {"tp": yy * 8 + zz * 2 + cc}

    pair, ynb = dev(y, z, 1 - c), dev(1 - y, z, c)
    rt, lf = dev(y, jnp.minimum(z + 1, 3), c), dev(y, jnp.maximum(z - 1, 0), c)
    z0, z1, z2, z3 = z == 0, z == 1, z == 2, z == 3
    end = jnp.logical_or(z0, z3)

    def row(k):
        return (k // NG) * BR

    def col(k, cc):
        return cc * 2048 + lax.rem(k, NG) * BC

    names_s = ["d2d", "yA", "zAR", "zAL", "zBR", "zBL", "yB", "fAl", "fAy", "fAz", "fBl", "fBy", "fBz",
               "gAR", "gAL", "gAyR", "gAyL", "gBy", "gBR", "gBL", "gp"]
    S = {n: ss.at[i] for i, n in enumerate(names_s)}
    names_r = ["yA", "zAR", "zAL", "zBR", "zBL", "yB", "gAR", "gAL", "gAyR", "gAyL", "gBy", "gBR0", "gBR1", "gBL0", "gBL1", "gp"]
    R = {n: (lambda k, i=i: rs.at[i, k]) for i, n in enumerate(names_r)}

    def oA(k, yy, rl, cc=c):
        return out.at[ds(row(k) + yy * 256 + rl * 128, 128), ds(col(k, cc), H)]

    def oB(k, rl, yy):
        return out.at[ds(row(k) + rl * 256 + yy * 128, 128), ds(col(k, c) + H, H)]

    def oB2(k, rl):
        return out.at[ds(row(k) + rl * 256, 256), ds(col(k, c) + H, H)]

    def st(ref):
        return lambda k: ref.at[lax.rem(k, DEPTH)]

    def rv(ref):
        return lambda k: ref.at[k]

    d2d = Chan(None, lambda k: d2d_st.at[lax.rem(k, 2)], lambda k: d2d_rv.at[lax.rem(k, 4)], S["d2d"],
               lambda k: d2d_r.at[lax.rem(k, 4)], pair, 2)
    yA = Chan(None, st(yA_st), rv(yA_rv), S["yA"], R["yA"], ynb)
    zA = [Chan(z < 3, st(zA_st.at[0]), rv(zA_rv.at[0]), S["zAR"], R["zAR"], rt),
          Chan(z > 0, st(zA_st.at[1]), rv(zA_rv.at[1]), S["zAL"], R["zAL"], lf)]
    zB = [Chan(z < 3, st(zB_st.at[0]), rv(zB_rv.at[0]), S["zBR"], R["zBR"], rt),
          Chan(z > 0, st(zB_st.at[1]), rv(zB_rv.at[1]), S["zBL"], R["zBL"], lf)]
    yB = Chan(end, st(yB_st), rv(yB_rv), S["yB"], R["yB"], ynb)
    fA, fB, gA, gAy, gB = [], [], [], [], []
    for rl, (fin, back, recvs) in enumerate(((z3, lf, ("gAR", "gAyR")), (z0, rt, ("gAL", "gAyL")))):
        o = lambda k, rl=rl: oA(k, y, rl)
        fA.append([Chan(fin, st(fA_st), o, S["fAl"]),
                   Chan(fin, st(fA_st), o, S["fAy"], R[recvs[1]], ynb),
                   Chan(fin, st(fA_st), o, S["fAz"], R[recvs[0]], back)])
        mid = jnp.logical_or(z1, z2)
        gA.append(Chan(mid, o, o, S["gAR" if rl == 0 else "gAL"], R[recvs[0]], back))
        nf = (z < 3) if rl == 0 else (z > 0)
        gAy.append(Chan(nf, o, o, S["gAyR" if rl == 0 else "gAyL"], R[recvs[1]], ynb))
        ob = lambda k, rl=rl: oB(k, rl, y)
        ob_other = lambda k, rl=rl: oB(k, rl, 1 - y)
        nm = "gBR" if rl == 0 else "gBL"
        by_y = lambda me, nm=nm: (lambda k: rs.at[names_r.index(nm + "0") + me, k])
        fB.append([Chan(fin, st(fB_st), ob, S["fBl"]),
                   Chan(fin, st(fB_st), ob, S["fBy"], R["gBy"], ynb),
                   Chan(fin, st(fB_st), ob, S["fBz"], by_y(y), back),
                   Chan(fin, ob_other, ob_other, S["gBy"], by_y(1 - y), back)])
        ob2 = lambda k, rl=rl: oB2(k, rl)
        gB.append(Chan(mid, ob2, ob2, S[nm], R[nm + "0"], back))
    whole = lambda k: out.at[ds(row(k), BR), ds(col(k, c), BC)]
    gp = Chan(None, whole, whole, S["gp"], R["gp"], pair)

    def got(dst, sem):
        pltpu.make_async_copy(dst, dst, sem).wait()

    pltpu.make_async_copy(wd_h, wd, ld.at[0]).start()

    def blk(b):
        r = ds(b * BR, BR)
        return [pltpu.make_async_copy(dy.at[r], dyb, ld.at[3]),
                pltpu.make_async_copy(gate.at[r], gb, ld.at[4]),
                pltpu.make_async_copy(up.at[r], ub, ld.at[5])]

    for cp in blk(0):
        cp.start()
    pltpu.make_async_copy(wg_h, wg, ld.at[1]).start()
    pltpu.make_async_copy(wu_h, wu, ld.at[2]).start()
    pltpu.make_async_copy(wd_h, wd, ld.at[0]).wait()

    def tile(j):
        s = lax.rem(j, 2)
        return [pltpu.make_async_copy(x.at[:, ds(j * TW, TW)], wg.at[ds(s * 2048, 2048), pl.ds(0, TW)], tl.at[0, s]),
                pltpu.make_async_copy(dy.at[:, ds(j * TW, TW)], wg.at[ds(s * 2048, 2048), pl.ds(TW, TW)], tl.at[1, s])]

    def tile_out(j):
        s = lax.rem(j, 2)
        return [pltpu.make_async_copy(o_gu.at[s, :, pl.ds(0, F)], dwg.at[ds(j * TW, TW)], tl.at[2, s]),
                pltpu.make_async_copy(o_gu.at[s, :, pl.ds(F, F)], dwu.at[ds(j * TW, TW)], tl.at[3, s]),
                pltpu.make_async_copy(o_d.at[s], dwd.at[:, ds(j * TW, TW)], tl.at[4, s])]

    def hidden_block(b):
        for cp in blk(b):
            cp.wait()
        r = ds(b * BR, BR)

        @pl.loop(0, F // 256)
        def _(n):
            f = ds(n * 256, 256)
            dh = mm(dyb[...], wd[f, :], NT)
            g, u = gb[:, f].astype(F32), ub[:, f].astype(F32)
            sig = jax.nn.sigmoid(g)
            silu = g * sig
            hT[f, r] = (silu * u).T.astype(BF16)
            dgu[r, f] = (dh * u * (sig + silu * (1.0 - sig))).astype(BF16)
            dgu[r, ds(F + n * 256, 256)] = (dh * silu).astype(BF16)

        @pl.when(b + 1 < ROWS // BR)
        def _():
            for cp in blk(b + 1):
                cp.start()

    def term(k, cols):
        r = ds(row(k), BR)
        return mm(dgu[r, pl.ds(0, F)], wg[cols, :], NT) + mm(dgu[r, pl.ds(F, F)], wu[cols, :], NT)

    def a0(k):
        @pl.when(lax.rem(k, NG) == 0)
        def _():
            hidden_block(k // NG)

        @pl.when(k == 0)
        def _():
            pltpu.make_async_copy(wg_h, wg, ld.at[1]).wait()
            pltpu.make_async_copy(wu_h, wu, ld.at[2]).wait()

        d2d.ready(k)
        for h in range(2):
            d2d_st[lax.rem(k, 2), :, pl.ds(h * H, H)] = term(k, ds(col(k, 1 - c) + h * H, H)).astype(BF16)

        @pl.when(k >= 4)
        def _():
            pl.semaphore_wait(credit, 1)

        d2d.start(k)

    def a1(k):
        s, q = lax.rem(k, NA), lax.rem(k, DEPTH)
        s4 = lax.rem(k, 4)
        got(d2d_rv.at[s4], d2d_r.at[s4])
        yA.ready(k)
        tmp[...] = term(k, ds(col(k, c), H)) + d2d_rv[s4, :, pl.ds(0, H)].astype(F32)
        yA_st[q] = tmp[ds((1 - y) * 256, 256), :].astype(BF16)
        yA.start(k)
        accA[s] = tmp[ds(y * 256, 256), :]
        accB[s] = term(k, ds(col(k, c) + H, H)) + d2d_rv[s4, :, pl.ds(H, H)].astype(F32)

        @pl.when(k < N - 4)
        def _():
            pl.semaphore_signal(credit, 1, device_id=pair, device_id_type=pl.DeviceIdType.MESH)

        for rl, first in ((0, z0), (1, z3)):
            @pl.when(first)
            def _():
                zB[rl].ready(k)
                zB_st[rl, q] = accB[s, pl.ds(rl * 256, 256), :].astype(BF16)
                zB[rl].start(k)

    def passA(k, rl):
        s, q = lax.rem(k, NA), lax.rem(k, DEPTH)
        got(zA_rv.at[rl, k], R["zAR" if rl == 0 else "zAL"](k))
        zA[rl].ready(k)
        zA_st[rl, q] = (accA[s, pl.ds(rl * 128, 128), :] + zA_rv[rl, k].astype(F32)).astype(BF16)
        zA[rl].start(k)

    def passB(k, rl):
        s, q = lax.rem(k, NA), lax.rem(k, DEPTH)
        got(zB_rv.at[rl, k], R["zBR" if rl == 0 else "zBL"](k))
        zB[rl].ready(k)
        zB_st[rl, q] = (accB[s, pl.ds(rl * 256, 256), :] + zB_rv[rl, k].astype(F32)).astype(BF16)
        zB[rl].start(k)

    def a2(k):
        s, q = lax.rem(k, NA), lax.rem(k, DEPTH)
        pl.when(z1)(lambda: passB(k, 0))
        pl.when(z2)(lambda: passB(k, 1))
        got(yA_rv.at[k], R["yA"](k))
        accA[s] = accA[s] + yA_rv[k].astype(F32)
        for rl, first in ((0, z0), (1, z3)):
            @pl.when(first)
            def _():
                zA[rl].ready(k)
                zA_st[rl, q] = accA[s, pl.ds(rl * 128, 128), :].astype(BF16)
                zA[rl].start(k)

    def a3(k):
        pl.when(z2)(lambda: passB(k, 0))
        pl.when(z1)(lambda: passB(k, 1))
        pl.when(z1)(lambda: passA(k, 0))
        pl.when(z2)(lambda: passA(k, 1))

    def a4(k):
        s, q = lax.rem(k, NA), lax.rem(k, DEPTH)
        for rl, fin in ((0, z3), (1, z0)):
            @pl.when(fin)
            def _():
                got(zB_rv.at[rl, k], R["zBR" if rl == 0 else "zBL"](k))
                yB.ready(k)
                r = pl.ds(rl * 256, 256)
                accB[s, r, :] = accB[s, r, :] + zB_rv[rl, k].astype(F32)
                yB_st[q] = accB[s, ds(rl * 256 + (1 - y) * 128, 128), :].astype(BF16)
                yB.start(k)
        pl.when(z2)(lambda: passA(k, 0))
        pl.when(z1)(lambda: passA(k, 1))

    def a5(k):
        s, q = lax.rem(k, NA), lax.rem(k, DEPTH)
        for rl, fin in ((0, z3), (1, z0)):
            @pl.when(fin)
            def _():
                got(yB_rv.at[k], R["yB"](k))
                for ch in fB[rl][:3]:
                    ch.ready(k)
                fB_st[q] = (accB[s, ds(rl * 256 + y * 128, 128), :] + yB_rv[k].astype(F32)).astype(BF16)
                for ch in fB[rl][:3]:
                    ch.start(k)
                got(zA_rv.at[rl, k], R["zAR" if rl == 0 else "zAL"](k))
                for ch in fA[rl]:
                    ch.ready(k)
                fA_st[q] = (accA[s, pl.ds(rl * 128, 128), :] + zA_rv[rl, k].astype(F32)).astype(BF16)
                for ch in fA[rl]:
                    ch.start(k)

    def fwdA(k, rl, z_too):
        got(oA(k, y, rl), R["gAR" if rl == 0 else "gAL"](k))
        if z_too:
            gA[rl].go(k)
        gAy[rl].go(k)

    def a6(k):
        pl.when(z2)(lambda: fwdA(k, 0, True))
        pl.when(z1)(lambda: fwdA(k, 1, True))
        for rl, fin in ((0, z3), (1, z0)):
            @pl.when(fin)
            def _():
                fA[rl][0].desc(k).wait()
                fB[rl][0].desc(k).wait()
                got(oB(k, rl, 1 - y), R["gBy"](k))
                fB[rl][3].go(k)

    def a7(k):
        pl.when(z1)(lambda: fwdA(k, 0, True))
        pl.when(z2)(lambda: fwdA(k, 1, True))
        for rl, m in ((0, z2), (1, z1)):
            @pl.when(m)
            def _():
                nm = "gBR" if rl == 0 else "gBL"
                for yy in range(2):
                    got(oB(k, rl, yy), R[nm + str(yy)](k))
                gB[rl].go(k)

    def a8(k):
        pl.when(z0)(lambda: fwdA(k, 0, False))
        pl.when(z3)(lambda: fwdA(k, 1, False))
        for rl, m in ((0, z1), (1, z2)):
            @pl.when(m)
            def _():
                got(oB2(k, rl), R["gBR0" if rl == 0 else "gBL0"](k))
                gB[rl].go(k)

    def a9(k):
        for rl, m in enumerate((z0, z3)):
            @pl.when(m)
            def _():
                got(oB2(k, rl), R["gBR0" if rl == 0 else "gBL0"](k))
            got(oA(k, 1 - y, rl), R["gAyR" if rl == 0 else "gAyL"](k))
        gp.go(k)

    for rl in range(2):
        for ch in (fA[rl][0], fB[rl][0]):
            ch.ready = lambda k: None

    def weights(j):
        for cp in tile(j):
            cp.wait()

        @pl.when(j + 1 < NW)
        def _():
            for cp in tile(j + 1):
                cp.start()

        @pl.when(j >= 2)
        def _():
            for cp in tile_out(j - 2):
                cp.wait()

        s = lax.rem(j, 2)
        o_gu[s] = mm(wg[ds(s * 2048, 2048), pl.ds(0, TW)], dgu[...], TN).astype(BF16)
        o_d[s] = mm(hT[...], wg[ds(s * 2048, 2048), pl.ds(TW, TW)], (((1,), (0,)), ((), ()))).astype(BF16)
        for cp in tile_out(j):
            cp.start()

    stages = (a0, a1, a2, a3, a4, a5, a6, a7, a8, a9)

    @pl.loop(0, T)
    def _(t):
        for i in reversed(range(10)):
            k = t - OFF[i]

            @pl.when(jnp.logical_and(k >= 0, k < N))
            def _():
                stages[i](k)

        @pl.when(t == DW0 - 1)
        def _():
            for cp in tile(0):
                cp.start()

        j = t - DW0

        @pl.when(jnp.logical_and(j >= 0, j < NW))
        def _():
            weights(j)

    for j in (NW - 2, NW - 1):
        for cp in tile_out(j):
            cp.wait()
    d2d.drain(N)
    yA.drain(N)
    for ch in (*zA, *zB, yB, *fA[0][1:], *fA[1][1:], *fB[0][1:], *fB[1][1:], *gA, *gAy, *gB, gp):
        ch.drain(N)

    @pl.loop(0, N)
    def _(k):
        got(out.at[ds(row(k), BR), ds(col(k, 1 - c), BC)], R["gp"](k))


def solution(mesh):
    def step(x, dy, gate, up, w_gate, w_up, w_down):
        hbm = pl.BlockSpec(memory_space=pl.ANY)
        V, DMA = pltpu.VMEM, pltpu.SemaphoreType.DMA
        return pl.pallas_call(
            kernel,
            name="mlp_bwd",
            out_shape=[
                jax.ShapeDtypeStruct((ROWS, D), BF16),
                jax.ShapeDtypeStruct((D, F), BF16),
                jax.ShapeDtypeStruct((D, F), BF16),
                jax.ShapeDtypeStruct((F, D), BF16),
            ],
            in_specs=[hbm] * 7,
            out_specs=[hbm] * 4,
            scratch_shapes=[
                V((F, D), BF16), V((D, F), BF16), V((D, F), BF16),
                V((ROWS, 2 * F), BF16), V((F, ROWS), BF16),
                V((BR, D), BF16), V((BR, F), BF16), V((BR, F), BF16),
                V((2, BR, BC), BF16), V((4, BR, BC), BF16),
                V((BR, H), F32), V((NA, 256, H), F32), V((NA, 512, H), F32),
                V((N, 256, H), BF16), V((2, N, 128, H), BF16), V((2, N, 256, H), BF16), V((N, 128, H), BF16),
                V((DEPTH, 256, H), BF16), V((2, DEPTH, 128, H), BF16), V((2, DEPTH, 256, H), BF16), V((DEPTH, 128, H), BF16),
                V((DEPTH, 128, H), BF16), V((DEPTH, 128, H), BF16),
                V((2, TW, 2 * F), BF16), V((2, F, TW), BF16),
                DMA((6,)), DMA((5, 2)), DMA((21, DEPTH)), DMA((16, N)), DMA((4,)),
                pltpu.SemaphoreType.REGULAR,
            ],
            compiler_params=pltpu.CompilerParams(has_side_effects=True, vmem_limit_bytes=67043328),
            cost_estimate=pl.CostEstimate(flops=77_000_000_000, bytes_accessed=100_000_000, transcendentals=0),
        )(x, dy, gate, up, w_gate, w_up, w_down)

    tokens, columns, rows = P("dp", None), P(None, "tp"), P("tp", None)
    return jax.shard_map(
        step,
        mesh=mesh,
        in_specs=(tokens, tokens, P("dp", "tp"), P("dp", "tp"), columns, columns, rows),
        out_specs=(tokens, P("dp", "tp"), P("dp", "tp"), P(("dp", "tp"), None)),
        check_vma=False,
    )
```

```python
import functools

import jax
import jax.numpy as jnp
from jax import lax
from jax.experimental import pallas as pl
from jax.experimental.pallas import tpu as pltpu
from jax.sharding import PartitionSpec as P

F32, BF16 = jnp.float32, jnp.bfloat16
ROWS, D, F = 2048, 4096, 768
BR = 512
H = 256
NG = 2048 // H
N = (ROWS // BR) * NG
PAT = "ABABA"
PP = len(PAT)
CH = {r: [k for k in range(N) if PAT[k % PP] == r] for r in "AB"}
CNT = {r: len(CH[r]) for r in "AB"}
OFF = {"A": (0, 2, 7, 7, 10, 16, 17, 19, 31, 38), "B": (0, 2, 3, 5, 15, 20, 24, 26, 30, 38)}
ORDER = (9, 10, 2, 6, 4, 5, 8, 1, 3, 0, 7)
HS = (0, 5, 15, 20)
DW0 = 25
TW = 256
NW = D // TW
UP = PP - PP % 2
TT = max(-(-(N + OFF["A"][9]) // PP), DW0 // PP + 2 * NW // UP)


def turn(r, i, stage):
    return CH[r][i] + OFF[r][stage], ORDER.index(stage)


def slots(r):
    return next(n for n in range(1, CNT[r]) if all(turn(r, i + n, 1) > turn(r, i, 5) for i in range(CNT[r] - n)))


NS = {r: slots(r) for r in "AB"}
DEPTH = 4
DR = 8
NT = (((1,), (1,)), ((), ()))
TN = (((0,), (0,)), ((), ()))
NN = (((1,), (0,)), ((), ()))


def mm(a, b, dims):
    return lax.dot_general(a, b, dims, preferred_element_type=F32)


def ds(start, size):
    return pl.ds(pl.multiple_of(start, size), size)


class Chan:
    def __init__(self, n, cond, src, dst, send, recv=None, dev=None):
        self.n, self.cond, self.src, self.dst, self.send, self.recv, self.dev = n, cond, src, dst, send, recv, dev

    def desc(self, k, i):
        sem = self.send.at[lax.rem(i, DEPTH)]
        if self.dev is None:
            return pltpu.make_async_copy(self.src(k, i), self.dst(k, i), sem)
        return pltpu.make_async_remote_copy(
            self.src(k, i), self.dst(k, i), sem, self.recv(i), device_id=self.dev, device_id_type=pl.DeviceIdType.MESH
        )

    def wait(self, k, i):
        if self.dev is None:
            self.desc(k, i).wait()
        else:
            self.desc(k, i).wait_send()

    def ready(self, k, i):
        @pl.when(i >= DEPTH)
        def _():
            self.wait(k, i)

    def start(self, k, i):
        self.desc(k, i).start()

    def go(self, k, i):
        self.ready(k, i)
        self.start(k, i)

    def drain(self):
        def run():
            @pl.loop(self.n - DEPTH, self.n)
            def _(i):
                self.wait(0, i)

        if self.cond is None:
            run()
        else:
            pl.when(self.cond)(run)


def kernel(x, dy, gate, up, wg_h, wu_h, wd_h, out, dwg, dwu, dwd,
           wd, wg, wu, dgu, hT, xb, gb, ub, d2d_st, d2d_rv, tmp, accA, accB,
           yA_rv, zA_rv, zB_rv, yB_rv, yA_st, zA_st, zB_st, yB_st, fA_st, fB_st, o_gu, o_d,
           ld, tl, ss, rs, credit):
    tp = lax.axis_index("tp")
    y, z, c = tp // 8, lax.rem(tp // 2, 4), lax.rem(tp, 2)

    def dev(yy, zz, cc):
        return {"tp": yy * 8 + zz * 2 + cc}

    pair, ynb = dev(y, z, 1 - c), dev(1 - y, z, c)
    rt, lf = dev(y, jnp.minimum(z + 1, 3), c), dev(y, jnp.maximum(z - 1, 0), c)
    z0, z1, z2, z3 = z == 0, z == 1, z == 2, z == 3
    mid = jnp.logical_or(z1, z2)
    end = jnp.logical_or(z0, z3)
    nA, nB = CNT["A"], CNT["B"]

    def row(k):
        return (k // NG) * BR

    def col(k, cc):
        return cc * 2048 + lax.rem(k, NG) * H

    names_s = ["d2d", "yA", "zAR", "zAL", "zBR", "zBL", "yB", "fAl", "fAy", "fAz", "fBl", "fBy", "fBz",
               "gAR", "gAL", "gAyR", "gAyL", "gBy", "gBR", "gBL", "gp"]
    S = {n: ss.at[i] for i, n in enumerate(names_s)}
    names_r = ["yA", "zAR", "zAL", "zBR", "zBL", "yB", "gAR", "gAL", "gAyR", "gAyL", "gBy",
               "gBR0", "gBR1", "gBL0", "gBL1", "gp", "d2d"]
    R = {n: (lambda i, j=j: rs.at[j, i]) for j, n in enumerate(names_r)}

    def oA(k, yy, rl):
        return out.at[ds(row(k) + yy * 256 + rl * 128, 128), ds(col(k, c), H)]

    def oB(k, rl, yy):
        return out.at[ds(row(k) + rl * 256 + yy * 128, 128), ds(col(k, c), H)]

    def oB2(k, rl):
        return out.at[ds(row(k) + rl * 256, 256), ds(col(k, c), H)]

    def st(ref):
        return lambda k, i: ref.at[lax.rem(i, DEPTH)]

    def rv(ref):
        return lambda k, i: ref.at[i]

    d2d = Chan(N, None, st(d2d_st), lambda k, i: d2d_rv.at[lax.rem(i, DR)], S["d2d"],
               lambda i: R["d2d"](lax.rem(i, DR)), pair)
    yA = Chan(nA, None, st(yA_st), rv(yA_rv), S["yA"], R["yA"], ynb)
    zA = [Chan(nA, z < 3, st(zA_st.at[0]), rv(zA_rv.at[0]), S["zAR"], R["zAR"], rt),
          Chan(nA, z > 0, st(zA_st.at[1]), rv(zA_rv.at[1]), S["zAL"], R["zAL"], lf)]
    zB = [Chan(nB, z < 3, st(zB_st.at[0]), rv(zB_rv.at[0]), S["zBR"], R["zBR"], rt),
          Chan(nB, z > 0, st(zB_st.at[1]), rv(zB_rv.at[1]), S["zBL"], R["zBL"], lf)]
    yB = Chan(nB, end, st(yB_st), rv(yB_rv), S["yB"], R["yB"], ynb)
    fA, fB, gA, gAy, gB, loc = [], [], [], [], [], []
    for rl, (fin, back, recvs) in enumerate(((z3, lf, ("gAR", "gAyR")), (z0, rt, ("gAL", "gAyL")))):
        o = lambda k, i, rl=rl: oA(k, y, rl)
        fA.append([Chan(nA, fin, st(fA_st), o, S["fAy"], R[recvs[1]], ynb),
                   Chan(nA, fin, st(fA_st), o, S["fAz"], R[recvs[0]], back)])
        gA.append(Chan(nA, mid, o, o, S["gAR" if rl == 0 else "gAL"], R[recvs[0]], back))
        nf = (z < 3) if rl == 0 else (z > 0)
        gAy.append(Chan(nA, nf, o, o, S["gAyR" if rl == 0 else "gAyL"], R[recvs[1]], ynb))
        ob = lambda k, i, rl=rl: oB(k, rl, y)
        ob_other = lambda k, i, rl=rl: oB(k, rl, 1 - y)
        nm = "gBR" if rl == 0 else "gBL"
        by_y = lambda me, nm=nm: (lambda i: rs.at[names_r.index(nm + "0") + me, i])
        fB.append([Chan(nB, fin, st(fB_st), ob, S["fBy"], R["gBy"], ynb),
                   Chan(nB, fin, st(fB_st), ob, S["fBz"], by_y(y), back),
                   Chan(nB, fin, ob_other, ob_other, S["gBy"], by_y(1 - y), back)])
        ob2 = lambda k, i, rl=rl: oB2(k, rl)
        gB.append(Chan(nB, mid, ob2, ob2, S[nm], R[nm + "0"], back))
        loc.append((Chan(nA, fin, st(fA_st), o, S["fAl"]), Chan(nB, fin, st(fB_st), ob, S["fBl"])))
    whole = lambda k, i: out.at[ds(row(k), BR), ds(col(k, c), H)]
    gp = Chan(N, None, whole, whole, S["gp"], R["gp"], pair)

    def got(dst, sem):
        pltpu.make_async_copy(dst, dst, sem).wait()

    def dy_block(b):
        r = ds(b * BR, BR)
        cps = [pltpu.make_async_copy(dy.at[r, pl.ds(p * 256, 256)], xb.at[p // 4, pl.ds((p % 4) * 512, 512)], ld.at[3])
               for p in range(16)]
        return cps + [pltpu.make_async_copy(gate.at[r], gb, ld.at[4]), pltpu.make_async_copy(up.at[r], ub, ld.at[5])]

    def wd_part(n):
        return pltpu.make_async_copy(wd_h.at[ds(n * 256, 256)], wd.at[ds(n * 256, 256)], ld.at[6 + n])

    wd_part(0).start()
    for cp in dy_block(0):
        cp.start()
    wd_part(1).start()
    wd_part(2).start()
    pltpu.make_async_copy(wg_h, wg, ld.at[1]).start()
    pltpu.make_async_copy(wu_h, wu, ld.at[2]).start()

    def tile(kind, j):
        s = lax.rem(j, 2)
        return pltpu.make_async_copy((x, dy)[kind].at[:, ds(j * TW, TW)], xb.at[2 * kind + s], tl.at[kind, s])

    def tile_out(kind, j):
        s = lax.rem(j, 2)
        if kind == 0:
            return [pltpu.make_async_copy(o_gu.at[s, :, pl.ds(0, F)], dwg.at[ds(j * TW, TW)], tl.at[2, s]),
                    pltpu.make_async_copy(o_gu.at[s, :, pl.ds(F, F)], dwu.at[ds(j * TW, TW)], tl.at[3, s])]
        return [pltpu.make_async_copy(o_d.at[s], dwd.at[:, ds(j * TW, TW)], tl.at[4, s])]

    def hidden_block(b):
        got(xb, ld.at[3])
        got(gb, ld.at[4])
        got(ub, ld.at[5])
        r = ds(b * BR, BR)

        @pl.loop(0, F // 256)
        def _(n):
            pl.when(b == 0)(lambda: wd_part(n).wait())
            f = ds(n * 256, 256)
            dh = sum(mm(xb[p // 4, pl.ds((p % 4) * 512, 512), :], wd[f, pl.ds(p * 256, 256)], NT) for p in range(16))
            g, u = gb[:, f].astype(F32), ub[:, f].astype(F32)
            sig = jax.nn.sigmoid(g)
            silu = g * sig
            hT[f, r] = (silu * u).T.astype(BF16)
            dgu[r, f] = (dh * u * (sig + silu * (1.0 - sig))).astype(BF16)
            dgu[r, ds(F + n * 256, 256)] = (dh * silu).astype(BF16)

        @pl.when(b + 1 < ROWS // BR)
        def _():
            for cp in dy_block(b + 1):
                cp.start()

        @pl.when(b + 1 == ROWS // BR)
        def _():
            tile(0, 0).start()
            tile(1, 0).start()

    def term(k, cols):
        r = ds(row(k), BR)
        return mm(dgu[r, pl.ds(0, F)], wg[cols, :], NT) + mm(dgu[r, pl.ds(F, F)], wu[cols, :], NT)

    def a0(k, i, cls):
        @pl.when(k == 0)
        def _():
            pltpu.make_async_copy(wg_h, wg, ld.at[1]).wait()
            pltpu.make_async_copy(wu_h, wu, ld.at[2]).wait()

        d2d.ready(k, k)
        d2d_st[lax.rem(k, DEPTH)] = term(k, ds(col(k, 1 - c), H)).astype(BF16)

        @pl.when(k >= DR)
        def _():
            pl.semaphore_wait(credit, 1)

        d2d.start(k, k)

    def a1(k, i, cls):
        s, q, s8 = lax.rem(i, NS[cls]), lax.rem(i, DEPTH), lax.rem(k, DR)
        got(d2d_rv.at[s8], R["d2d"](s8))
        if cls == "A":
            yA.ready(k, i)
            tmp[...] = term(k, ds(col(k, c), H)) + d2d_rv[s8].astype(F32)
            yA_st[q] = tmp[ds((1 - y) * 256, 256), :].astype(BF16)
            yA.start(k, i)
            accA[s] = tmp[ds(y * 256, 256), :]
        else:
            accB[s] = term(k, ds(col(k, c), H)) + d2d_rv[s8].astype(F32)
            for rl, first in ((0, z0), (1, z3)):
                @pl.when(first)
                def _():
                    zB[rl].ready(k, i)
                    zB_st[rl, q] = accB[s, pl.ds(rl * 256, 256), :].astype(BF16)
                    zB[rl].start(k, i)

        @pl.when(k < N - DR)
        def _():
            pl.semaphore_signal(credit, 1, device_id=pair, device_id_type=pl.DeviceIdType.MESH)

    def passA(k, i, rl):
        s, q = lax.rem(i, NS["A"]), lax.rem(i, DEPTH)
        got(zA_rv.at[rl, i], R["zAR" if rl == 0 else "zAL"](i))
        zA[rl].ready(k, i)
        zA_st[rl, q] = (accA[s, pl.ds(rl * 128, 128), :] + zA_rv[rl, i].astype(F32)).astype(BF16)
        zA[rl].start(k, i)

    def passB(k, i, rl):
        s, q = lax.rem(i, NS["B"]), lax.rem(i, DEPTH)
        got(zB_rv.at[rl, i], R["zBR" if rl == 0 else "zBL"](i))
        zB[rl].ready(k, i)
        zB_st[rl, q] = (accB[s, pl.ds(rl * 256, 256), :] + zB_rv[rl, i].astype(F32)).astype(BF16)
        zB[rl].start(k, i)

    def a2(k, i, cls):
        s, q = lax.rem(i, NS[cls]), lax.rem(i, DEPTH)
        if cls == "B":
            pl.when(z1)(lambda: passB(k, i, 0))
            pl.when(z2)(lambda: passB(k, i, 1))
            return
        got(yA_rv.at[i], R["yA"](i))
        accA[s] = accA[s] + yA_rv[i].astype(F32)
        for rl, first in ((0, z0), (1, z3)):
            @pl.when(first)
            def _():
                zA[rl].ready(k, i)
                zA_st[rl, q] = accA[s, pl.ds(rl * 128, 128), :].astype(BF16)
                zA[rl].start(k, i)

    def a3(k, i, cls):
        if cls == "B":
            pl.when(z2)(lambda: passB(k, i, 0))
            pl.when(z1)(lambda: passB(k, i, 1))
        else:
            pl.when(z1)(lambda: passA(k, i, 0))
            pl.when(z2)(lambda: passA(k, i, 1))

    def a4(k, i, cls):
        s, q = lax.rem(i, NS[cls]), lax.rem(i, DEPTH)
        if cls == "A":
            pl.when(z2)(lambda: passA(k, i, 0))
            pl.when(z1)(lambda: passA(k, i, 1))
            return
        for rl, fin in ((0, z3), (1, z0)):
            @pl.when(fin)
            def _():
                got(zB_rv.at[rl, i], R["zBR" if rl == 0 else "zBL"](i))
                yB.ready(k, i)
                r = pl.ds(rl * 256, 256)
                accB[s, r, :] = accB[s, r, :] + zB_rv[rl, i].astype(F32)
                yB_st[q] = accB[s, ds(rl * 256 + (1 - y) * 128, 128), :].astype(BF16)
                yB.start(k, i)

    def a5(k, i, cls):
        s, q = lax.rem(i, NS[cls]), lax.rem(i, DEPTH)
        for rl, fin in ((0, z3), (1, z0)):
            @pl.when(fin)
            def _():
                if cls == "B":
                    got(yB_rv.at[i], R["yB"](i))
                    for ch in fB[rl][:2]:
                        ch.ready(k, i)
                    fB_st[q] = (accB[s, ds(rl * 256 + y * 128, 128), :] + yB_rv[i].astype(F32)).astype(BF16)
                    for ch in (*fB[rl][:2], loc[rl][1]):
                        ch.start(k, i)
                else:
                    got(zA_rv.at[rl, i], R["zAR" if rl == 0 else "zAL"](i))
                    for ch in fA[rl]:
                        ch.ready(k, i)
                    fA_st[q] = (accA[s, pl.ds(rl * 128, 128), :] + zA_rv[rl, i].astype(F32)).astype(BF16)
                    for ch in (*fA[rl], loc[rl][0]):
                        ch.start(k, i)

    def fwdA(k, i, rl, z_too):
        got(oA(k, y, rl), R["gAR" if rl == 0 else "gAL"](i))
        if z_too:
            gA[rl].go(k, i)
        gAy[rl].go(k, i)

    def a6(k, i, cls):
        if cls == "A":
            pl.when(z2)(lambda: fwdA(k, i, 0, True))
            pl.when(z1)(lambda: fwdA(k, i, 1, True))
            return
        for rl, fin in ((0, z3), (1, z0)):
            @pl.when(fin)
            def _():
                got(oB(k, rl, 1 - y), R["gBy"](i))
                fB[rl][2].go(k, i)

    def a7(k, i, cls):
        if cls == "A":
            pl.when(z1)(lambda: fwdA(k, i, 0, True))
            pl.when(z2)(lambda: fwdA(k, i, 1, True))
            return
        for rl, m in ((0, z2), (1, z1)):
            @pl.when(m)
            def _():
                nm = "gBR" if rl == 0 else "gBL"
                for yy in range(2):
                    got(oB(k, rl, yy), R[nm + str(yy)](i))
                gB[rl].go(k, i)

    def a8(k, i, cls):
        if cls == "A":
            pl.when(z0)(lambda: fwdA(k, i, 0, False))
            pl.when(z3)(lambda: fwdA(k, i, 1, False))
            return
        for rl, m in ((0, z1), (1, z2)):
            @pl.when(m)
            def _():
                got(oB2(k, rl), R["gBR0" if rl == 0 else "gBL0"](i))
                gB[rl].go(k, i)

    def a9(k, i, cls):
        for rl, m in enumerate((z0, z3)):
            if cls == "B":
                @pl.when(m)
                def _():
                    got(oB2(k, rl), R["gBR0" if rl == 0 else "gBL0"](i))
            else:
                got(oA(k, 1 - y, rl), R["gAyR" if rl == 0 else "gAyL"](i))
        gp.go(k, k)

    def weights(kind, j):
        tile(kind, j).wait()

        @pl.when(j + 1 < NW)
        def _():
            tile(kind, j + 1).start()

        @pl.when(j >= 2)
        def _():
            for cp in tile_out(kind, j - 2):
                cp.wait()

        s = lax.rem(j, 2)
        if kind == 0:
            o_gu[s] = mm(xb[s], dgu[...], TN).astype(BF16)
        else:
            o_d[s] = mm(hT[...], xb[2 + s], NN).astype(BF16)
        for cp in tile_out(kind, j):
            cp.start()

    stages = (a0, a1, a2, a3, a4, a5, a6, a7, a8, a9)

    def settle(k, i, cls):
        for rl, fin in ((0, z3), (1, z0)):
            pl.when(fin)(lambda: loc[rl]["AB".index(cls)].wait(k, i))

    @pl.loop(0, TT)
    def _(tt):
        for par in range(PP):
            t = tt * PP + par

            def chunk(cls, stage, run):
                ph = (par - OFF[cls][stage]) % PP
                if PAT[ph] != cls:
                    return
                rnd = tt + (par - OFF[cls][stage] - ph) // PP
                k, i = rnd * PP + ph, rnd * PAT.count(cls) + PAT[:ph].count(cls)

                @pl.when(jnp.logical_and(k >= 0, k < N))
                def _():
                    run(k, i, cls)

            if par == 0:
                b = sum((t >= s).astype(jnp.int32) for s in HS[1:])
                pl.when(functools.reduce(jnp.logical_or, [t == s for s in HS]))(lambda: hidden_block(b))
            for stage in ORDER:
                if stage == 0:
                    pl.when(t < N)(lambda: a0(t, t, None))
                elif stage == 10:
                    j = (tt - DW0 // PP) * (UP // 2) + par // 2

                    if par < UP:
                        @pl.when(jnp.logical_and(tt >= DW0 // PP, j < NW))
                        def _():
                            weights(par % 2, j)
                else:
                    for cls in "AB":
                        chunk(cls, stage, stages[stage])
            for cls in "AB":
                chunk(cls, 5, settle)

    for kind in range(2):
        for j in (NW - 2, NW - 1):
            for cp in tile_out(kind, j):
                cp.wait()
    for ch in (d2d, yA, *zA, *zB, yB, *fA[0], *fA[1], *fB[0], *fB[1], *gA, *gAy, *gB, gp):
        ch.drain()

    @pl.loop(0, N)
    def _(k):
        got(out.at[ds(row(k), BR), ds(col(k, 1 - c), H)], R["gp"](k))


def solution(mesh):
    def step(x, dy, gate, up, w_gate, w_up, w_down):
        hbm = pl.BlockSpec(memory_space=pl.ANY)
        V, DMA = pltpu.VMEM, pltpu.SemaphoreType.DMA
        return pl.pallas_call(
            kernel,
            name="mlp_bwd",
            out_shape=[
                jax.ShapeDtypeStruct((ROWS, D), BF16),
                jax.ShapeDtypeStruct((D, F), BF16),
                jax.ShapeDtypeStruct((D, F), BF16),
                jax.ShapeDtypeStruct((F, D), BF16),
            ],
            in_specs=[hbm] * 7,
            out_specs=[hbm] * 4,
            scratch_shapes=[
                V((F, D), BF16), V((D, F), BF16), V((D, F), BF16),
                V((ROWS, 2 * F), BF16), V((F, ROWS), BF16),
                V((4, ROWS, TW), BF16), V((BR, F), BF16), V((BR, F), BF16),
                V((DEPTH, BR, H), BF16), V((DR, BR, H), BF16),
                V((BR, H), F32), V((NS["A"], 256, H), F32), V((NS["B"], 512, H), F32),
                V((CNT["A"], 256, H), BF16), V((2, CNT["A"], 128, H), BF16),
                V((2, CNT["B"], 256, H), BF16), V((CNT["B"], 128, H), BF16),
                V((DEPTH, 256, H), BF16), V((2, DEPTH, 128, H), BF16), V((2, DEPTH, 256, H), BF16), V((DEPTH, 128, H), BF16),
                V((DEPTH, 128, H), BF16), V((DEPTH, 128, H), BF16),
                V((2, TW, 2 * F), BF16), V((2, F, TW), BF16),
                DMA((9,)), DMA((5, 2)), DMA((21, DEPTH)), DMA((17, N)),
                pltpu.SemaphoreType.REGULAR,
            ],
            compiler_params=pltpu.CompilerParams(has_side_effects=True, vmem_limit_bytes=67043328),
            cost_estimate=pl.CostEstimate(flops=77_000_000_000, bytes_accessed=100_000_000, transcendentals=0),
        )(x, dy, gate, up, w_gate, w_up, w_down)

    tokens, columns, rows = P("dp", None), P(None, "tp"), P("tp", None)
    return jax.shard_map(
        step,
        mesh=mesh,
        in_specs=(tokens, tokens, P("dp", "tp"), P("dp", "tp"), columns, columns, rows),
        out_specs=(tokens, P("dp", "tp"), P("dp", "tp"), P(("dp", "tp"), None)),
        check_vma=False,
    )
```

```python
import functools

import jax
import jax.numpy as jnp
from jax import lax
from jax.experimental import pallas as pl
from jax.experimental.pallas import tpu as pltpu
from jax.sharding import PartitionSpec as P

F32, BF16 = jnp.float32, jnp.bfloat16
ROWS, D, F = 2048, 4096, 768
BR = 512
H = 256
NG = 2048 // H
N = (ROWS // BR) * NG
PAT = "AABAB"
PP = len(PAT)
CH = {r: [k for k in range(N) if PAT[k % PP] == r] for r in "AB"}
CNT = {r: len(CH[r]) for r in "AB"}
OFF = {"A": (0, 2, 7, 7, 10, 15, 17, 19, 31, 38), "B": (0, 2, 3, 5, 15, 20, 24, 26, 30, 38)}
ORDER = (10, 9, 2, 6, 4, 5, 8, 1, 3, 0, 7)
HS = (0, 5, 15, 20)
DW0 = 25
TW = 256
NW = D // TW
UP = PP - PP % 2
TT = max(-(-(N + OFF["A"][9]) // PP), DW0 // PP + 2 * NW // UP)


def turn(r, i, stage):
    return CH[r][i] + OFF[r][stage], ORDER.index(stage)


def slots(r):
    return next(n for n in range(1, CNT[r]) if all(turn(r, i + n, 1) > turn(r, i, 5) for i in range(CNT[r] - n)))


NS = {r: slots(r) for r in "AB"}
DEPTH = 4
DR = 8
WR, SR = 256, 1024
CR, CL = 8, 4
NT = (((1,), (1,)), ((), ()))
TN = (((0,), (0,)), ((), ()))
NN = (((1,), (0,)), ((), ()))


def mm(a, b, dims):
    return lax.dot_general(a, b, dims, preferred_element_type=F32)


def ds(start, size):
    return pl.ds(pl.multiple_of(start, size), size)


class Chan:
    def __init__(self, n, cond, src, dst, send, recv=None, dev=None):
        self.n, self.cond, self.src, self.dst, self.send, self.recv, self.dev = n, cond, src, dst, send, recv, dev

    def desc(self, k, i):
        sem = self.send.at[lax.rem(i, DEPTH)]
        if self.dev is None:
            return pltpu.make_async_copy(self.src(k, i), self.dst(k, i), sem)
        return pltpu.make_async_remote_copy(
            self.src(k, i), self.dst(k, i), sem, self.recv(i), device_id=self.dev, device_id_type=pl.DeviceIdType.MESH
        )

    def wait(self, k, i):
        if self.dev is None:
            self.desc(k, i).wait()
        else:
            self.desc(k, i).wait_send()

    def ready(self, k, i):
        @pl.when(i >= DEPTH)
        def _():
            self.wait(k, i)

    def start(self, k, i):
        self.desc(k, i).start()

    def go(self, k, i):
        self.ready(k, i)
        self.start(k, i)

    def drain(self):
        def run():
            @pl.loop(self.n - DEPTH, self.n)
            def _(i):
                self.wait(0, i)

        if self.cond is None:
            run()
        else:
            pl.when(self.cond)(run)


def kernel(x, dy, gate, up, wg_h, wu_h, wd_h, out, dwg, dwu, dwd,
           wd, wg, wu, dgu, hT, xb, gb, ub, d2d_st, d2d_rv, tmp, accA, accB,
           yA_rv, zA_rv, zB_rv, yB_rv, yA_st, zA_st, zB_st, yB_st, fA_st, fB_st, o_gu, o_d,
           ld, tl, ss, rs, credit):
    tp = lax.axis_index("tp")
    y, z, c = tp // 8, lax.rem(tp // 2, 4), lax.rem(tp, 2)

    def dev(yy, zz, cc):
        return {"tp": yy * 8 + zz * 2 + cc}

    pair, ynb = dev(y, z, 1 - c), dev(1 - y, z, c)
    rt, lf = dev(y, jnp.minimum(z + 1, 3), c), dev(y, jnp.maximum(z - 1, 0), c)
    z0, z1, z2, z3 = z == 0, z == 1, z == 2, z == 3
    mid = jnp.logical_or(z1, z2)
    end = jnp.logical_or(z0, z3)
    nA, nB = CNT["A"], CNT["B"]

    def row(k):
        return (k // NG) * BR

    def col(k, cc):
        return cc * 2048 + lax.rem(k, NG) * H

    names_s = ["d2d", "yA", "zAR", "zAL", "zBR", "zBL", "yB", "fAl", "fAy", "fAz", "fBl", "fBy", "fBz",
               "gAR", "gAL", "gAyR", "gAyL", "gBy", "gBR", "gBL", "gp"]
    S = {n: ss.at[i] for i, n in enumerate(names_s)}
    names_r = ["yA", "zAR", "zAL", "zBR", "zBL", "yB", "gAR", "gAL", "gAyR", "gAyL", "gBy",
               "gBR0", "gBR1", "gBL0", "gBL1", "gp", "d2d"]
    R = {n: (lambda i, j=j: rs.at[j, i]) for j, n in enumerate(names_r)}

    def oA(k, yy, rl):
        return out.at[ds(row(k) + yy * 256 + rl * 128, 128), ds(col(k, c), H)]

    def oB(k, rl, yy):
        return out.at[ds(row(k) + rl * 256 + yy * 128, 128), ds(col(k, c), H)]

    def oB2(k, rl):
        return out.at[ds(row(k) + rl * 256, 256), ds(col(k, c), H)]

    def st(ref):
        return lambda k, i: ref.at[lax.rem(i, DEPTH)]

    def rv(ref):
        return lambda k, i: ref.at[i]

    d2d = Chan(N, None, st(d2d_st), lambda k, i: d2d_rv.at[lax.rem(i, DR)], S["d2d"],
               lambda i: R["d2d"](lax.rem(i, DR)), pair)
    yA = Chan(nA, None, st(yA_st), rv(yA_rv), S["yA"], R["yA"], ynb)
    zA = [Chan(nA, z < 3, st(zA_st.at[0]), rv(zA_rv.at[0]), S["zAR"], R["zAR"], rt),
          Chan(nA, z > 0, st(zA_st.at[1]), rv(zA_rv.at[1]), S["zAL"], R["zAL"], lf)]
    zB = [Chan(nB, z < 3, st(zB_st.at[0]), rv(zB_rv.at[0]), S["zBR"], R["zBR"], rt),
          Chan(nB, z > 0, st(zB_st.at[1]), rv(zB_rv.at[1]), S["zBL"], R["zBL"], lf)]
    yB = Chan(nB, end, st(yB_st), rv(yB_rv), S["yB"], R["yB"], ynb)
    fA, fB, gA, gAy, gB, loc = [], [], [], [], [], []
    for rl, (fin, back, recvs) in enumerate(((z3, lf, ("gAR", "gAyR")), (z0, rt, ("gAL", "gAyL")))):
        o = lambda k, i, rl=rl: oA(k, y, rl)
        fA.append([Chan(nA, fin, st(fA_st), o, S["fAy"], R[recvs[1]], ynb),
                   Chan(nA, fin, st(fA_st), o, S["fAz"], R[recvs[0]], back)])
        gA.append(Chan(nA, mid, o, o, S["gAR" if rl == 0 else "gAL"], R[recvs[0]], back))
        nf = (z < 3) if rl == 0 else (z > 0)
        gAy.append(Chan(nA, nf, o, o, S["gAyR" if rl == 0 else "gAyL"], R[recvs[1]], ynb))
        ob = lambda k, i, rl=rl: oB(k, rl, y)
        ob_other = lambda k, i, rl=rl: oB(k, rl, 1 - y)
        nm = "gBR" if rl == 0 else "gBL"
        by_y = lambda me, nm=nm: (lambda i: rs.at[names_r.index(nm + "0") + me, i])
        fB.append([Chan(nB, fin, st(fB_st), ob, S["fBy"], R["gBy"], ynb),
                   Chan(nB, fin, st(fB_st), ob, S["fBz"], by_y(y), back),
                   Chan(nB, fin, ob_other, ob_other, S["gBy"], by_y(1 - y), back)])
        ob2 = lambda k, i, rl=rl: oB2(k, rl)
        gB.append(Chan(nB, mid, ob2, ob2, S[nm], R[nm + "0"], back))
        loc.append((Chan(nA, fin, st(fA_st), o, S["fAl"]), Chan(nB, fin, st(fB_st), ob, S["fBl"])))
    whole = lambda k, i: out.at[ds(row(k), BR), ds(col(k, c), H)]
    gp = Chan(N, None, whole, whole, S["gp"], R["gp"], pair)

    def got(dst, sem):
        pltpu.make_async_copy(dst, dst, sem).wait()

    def dy_block(b):
        r = ds(b * BR, BR)
        cps = [pltpu.make_async_copy(dy.at[r, pl.ds(p * 256, 256)], xb.at[p // 4, pl.ds((p % 4) * 512, 512)], ld.at[3])
               for p in range(16)]
        return cps + [pltpu.make_async_copy(gate.at[r], gb, ld.at[4]), pltpu.make_async_copy(up.at[r], ub, ld.at[5])]

    def wd_part(n):
        return pltpu.make_async_copy(wd_h.at[ds(n * 256, 256)], wd.at[ds(n * 256, 256)], ld.at[6 + n])

    wd_part(0).start()
    for cp in dy_block(0):
        cp.start()
    wd_part(1).start()
    wd_part(2).start()
    pltpu.make_async_copy(wg_h, wg, ld.at[1]).start()
    pltpu.make_async_copy(wu_h, wu, ld.at[2]).start()

    def tile(kind, j):
        s = lax.rem(j, 2)
        return pltpu.make_async_copy((x, dy)[kind].at[:, ds(j * TW, TW)], xb.at[2 * kind + s], tl.at[kind, s])

    def tile_out(kind, j):
        s = lax.rem(j, 2)
        if kind == 0:
            return [pltpu.make_async_copy(o_gu.at[s, :, pl.ds(0, F)], dwg.at[ds(j * TW, TW)], tl.at[2, s]),
                    pltpu.make_async_copy(o_gu.at[s, :, pl.ds(F, F)], dwu.at[ds(j * TW, TW)], tl.at[3, s])]
        return [pltpu.make_async_copy(o_d.at[s], dwd.at[:, ds(j * TW, TW)], tl.at[4, s])]

    def hidden_block(b):
        got(xb, ld.at[3])
        got(gb, ld.at[4])
        got(ub, ld.at[5])
        r = ds(b * BR, BR)

        @pl.loop(0, F // 256)
        def _(n):
            pl.when(b == 0)(lambda: wd_part(n).wait())
            f = ds(n * 256, 256)
            dh = sum(mm(xb[p // 4, pl.ds((p % 4) * 512, 512), :], wd[f, pl.ds(p * 256, 256)], NT) for p in range(16))
            g, u = gb[:, f].astype(F32), ub[:, f].astype(F32)
            sig = jax.nn.sigmoid(g)
            silu = g * sig
            hT[f, r] = (silu * u).T.astype(BF16)
            dgu[r, f] = (dh * u * (sig + silu * (1.0 - sig))).astype(BF16)
            dgu[r, ds(F + n * 256, 256)] = (dh * silu).astype(BF16)

        @pl.when(b + 1 < ROWS // BR)
        def _():
            for cp in dy_block(b + 1):
                cp.start()

        @pl.when(b + 1 == ROWS // BR)
        def _():
            tile(0, 0).start()
            tile(1, 0).start()

    def term(k, cols):
        r = ds(row(k), BR)
        return mm(dgu[r, pl.ds(0, F)], wg[cols, :], NT) + mm(dgu[r, pl.ds(F, F)], wu[cols, :], NT)

    def a0(k, i, cls):
        @pl.when(k == 0)
        def _():
            pltpu.make_async_copy(wg_h, wg, ld.at[1]).wait()
            pltpu.make_async_copy(wu_h, wu, ld.at[2]).wait()

        d2d.ready(k, k)
        d2d_st[lax.rem(k, DEPTH)] = term(k, ds(col(k, 1 - c), H)).astype(BF16)

        @pl.when(k >= DR)
        def _():
            pl.semaphore_wait(credit, 1)

        d2d.start(k, k)

    def a1(k, i, cls):
        s, q, s8 = lax.rem(i, NS[cls]), lax.rem(i, DEPTH), lax.rem(k, DR)
        got(d2d_rv.at[s8], R["d2d"](s8))
        if cls == "A":
            yA.ready(k, i)
            tmp[...] = term(k, ds(col(k, c), H)) + d2d_rv[s8].astype(F32)
            yA_st[q] = tmp[ds((1 - y) * 256, 256), :].astype(BF16)
            yA.start(k, i)
            accA[s] = tmp[ds(y * 256, 256), :]
        else:
            accB[s] = term(k, ds(col(k, c), H)) + d2d_rv[s8].astype(F32)
            for rl, first in ((0, z0), (1, z3)):
                @pl.when(first)
                def _():
                    zB[rl].ready(k, i)
                    zB_st[rl, q] = accB[s, pl.ds(rl * 256, 256), :].astype(BF16)
                    zB[rl].start(k, i)

        @pl.when(k < N - DR)
        def _():
            pl.semaphore_signal(credit, 1, device_id=pair, device_id_type=pl.DeviceIdType.MESH)

    def passA(k, i, rl):
        s, q = lax.rem(i, NS["A"]), lax.rem(i, DEPTH)
        got(zA_rv.at[rl, i], R["zAR" if rl == 0 else "zAL"](i))
        zA[rl].ready(k, i)
        zA_st[rl, q] = (accA[s, pl.ds(rl * 128, 128), :] + zA_rv[rl, i].astype(F32)).astype(BF16)
        zA[rl].start(k, i)

    def passB(k, i, rl):
        s, q = lax.rem(i, NS["B"]), lax.rem(i, DEPTH)
        got(zB_rv.at[rl, i], R["zBR" if rl == 0 else "zBL"](i))
        zB[rl].ready(k, i)
        zB_st[rl, q] = (accB[s, pl.ds(rl * 256, 256), :] + zB_rv[rl, i].astype(F32)).astype(BF16)
        zB[rl].start(k, i)

    def a2(k, i, cls):
        s, q = lax.rem(i, NS[cls]), lax.rem(i, DEPTH)
        if cls == "B":
            pl.when(z1)(lambda: passB(k, i, 0))
            pl.when(z2)(lambda: passB(k, i, 1))
            return
        got(yA_rv.at[i], R["yA"](i))
        accA[s] = accA[s] + yA_rv[i].astype(F32)
        for rl, first in ((0, z0), (1, z3)):
            @pl.when(first)
            def _():
                zA[rl].ready(k, i)
                zA_st[rl, q] = accA[s, pl.ds(rl * 128, 128), :].astype(BF16)
                zA[rl].start(k, i)

    def a3(k, i, cls):
        if cls == "B":
            pl.when(z2)(lambda: passB(k, i, 0))
            pl.when(z1)(lambda: passB(k, i, 1))
        else:
            pl.when(z1)(lambda: passA(k, i, 0))
            pl.when(z2)(lambda: passA(k, i, 1))

    def a4(k, i, cls):
        s, q = lax.rem(i, NS[cls]), lax.rem(i, DEPTH)
        if cls == "A":
            pl.when(z2)(lambda: passA(k, i, 0))
            pl.when(z1)(lambda: passA(k, i, 1))
            return
        for rl, fin in ((0, z3), (1, z0)):
            @pl.when(fin)
            def _():
                got(zB_rv.at[rl, i], R["zBR" if rl == 0 else "zBL"](i))
                yB.ready(k, i)
                r = pl.ds(rl * 256, 256)
                accB[s, r, :] = accB[s, r, :] + zB_rv[rl, i].astype(F32)
                yB_st[q] = accB[s, ds(rl * 256 + (1 - y) * 128, 128), :].astype(BF16)
                yB.start(k, i)

    def a5(k, i, cls):
        s, q = lax.rem(i, NS[cls]), lax.rem(i, DEPTH)
        for rl, fin in ((0, z3), (1, z0)):
            @pl.when(fin)
            def _():
                if cls == "B":
                    got(yB_rv.at[i], R["yB"](i))
                    for ch in fB[rl][:2]:
                        ch.ready(k, i)
                    fB_st[q] = (accB[s, ds(rl * 256 + y * 128, 128), :] + yB_rv[i].astype(F32)).astype(BF16)
                    for ch in (*fB[rl][:2], loc[rl][1]):
                        ch.start(k, i)
                else:
                    got(zA_rv.at[rl, i], R["zAR" if rl == 0 else "zAL"](i))
                    for ch in fA[rl]:
                        ch.ready(k, i)
                    fA_st[q] = (accA[s, pl.ds(rl * 128, 128), :] + zA_rv[rl, i].astype(F32)).astype(BF16)
                    for ch in (*fA[rl], loc[rl][0]):
                        ch.start(k, i)

    def fwdA(k, i, rl, z_too):
        got(oA(k, y, rl), R["gAR" if rl == 0 else "gAL"](i))
        if z_too:
            gA[rl].go(k, i)
        gAy[rl].go(k, i)

    def a6(k, i, cls):
        if cls == "A":
            pl.when(z2)(lambda: fwdA(k, i, 0, True))
            pl.when(z1)(lambda: fwdA(k, i, 1, True))
            return
        for rl, fin in ((0, z3), (1, z0)):
            @pl.when(fin)
            def _():
                got(oB(k, rl, 1 - y), R["gBy"](i))
                fB[rl][2].go(k, i)

    def a7(k, i, cls):
        if cls == "A":
            pl.when(z1)(lambda: fwdA(k, i, 0, True))
            pl.when(z2)(lambda: fwdA(k, i, 1, True))
            return
        for rl, m in ((0, z2), (1, z1)):
            @pl.when(m)
            def _():
                nm = "gBR" if rl == 0 else "gBL"
                for yy in range(2):
                    got(oB(k, rl, yy), R[nm + str(yy)](i))
                gB[rl].go(k, i)

    def a8(k, i, cls):
        if cls == "A":
            pl.when(z0)(lambda: fwdA(k, i, 0, False))
            pl.when(z3)(lambda: fwdA(k, i, 1, False))
            return
        for rl, m in ((0, z1), (1, z2)):
            @pl.when(m)
            def _():
                got(oB2(k, rl), R["gBR0" if rl == 0 else "gBL0"](i))
                gB[rl].go(k, i)

    def a9(k, i, cls):
        for rl, m in enumerate((z0, z3)):
            if cls == "B":
                @pl.when(m)
                def _():
                    got(oB2(k, rl), R["gBR0" if rl == 0 else "gBL0"](i))
            else:
                got(oA(k, 1 - y, rl), R["gAyR" if rl == 0 else "gAyL"](i))
        gp.go(k, k)

    def weights(kind, j):
        tile(kind, j).wait()

        @pl.when(j + 1 < NW)
        def _():
            tile(kind, j + 1).start()

        @pl.when(j >= 2)
        def _():
            for cp in tile_out(kind, j - 2):
                cp.wait()

        s = lax.rem(j, 2)
        if kind == 0:
            o_gu[s] = mm(xb[s], dgu[...], TN).astype(BF16)
        else:
            o_d[s] = mm(hT[...], xb[2 + s], NN).astype(BF16)
        for cp in tile_out(kind, j):
            cp.start()

    stages = (a0, a1, a2, a3, a4, a5, a6, a7, a8, a9)

    def settle(k, i, cls):
        for rl, fin in ((0, z3), (1, z0)):
            pl.when(fin)(lambda: loc[rl]["AB".index(cls)].wait(k, i))

    @pl.loop(0, TT)
    def _(tt):
        for par in range(PP):
            t = tt * PP + par

            def chunk(cls, stage, run):
                ph = (par - OFF[cls][stage]) % PP
                if PAT[ph] != cls:
                    return
                rnd = tt + (par - OFF[cls][stage] - ph) // PP
                k, i = rnd * PP + ph, rnd * PAT.count(cls) + PAT[:ph].count(cls)

                @pl.when(jnp.logical_and(k >= 0, k < N))
                def _():
                    run(k, i, cls)

            if par == 0:
                b = sum((t >= s).astype(jnp.int32) for s in HS[1:])
                pl.when(functools.reduce(jnp.logical_or, [t == s for s in HS]))(lambda: hidden_block(b))
            for stage in ORDER:
                if stage == 0:
                    pl.when(t < N)(lambda: a0(t, t, None))
                elif stage == 10:
                    j = (tt - DW0 // PP) * (UP // 2) + par // 2

                    if par < UP:
                        @pl.when(jnp.logical_and(tt >= DW0 // PP, j < NW))
                        def _():
                            weights(par % 2, j)
                else:
                    for cls in "AB":
                        chunk(cls, stage, stages[stage])
            for cls in "AB":
                chunk(cls, 5, settle)

    for kind in range(2):
        for j in (NW - 2, NW - 1):
            for cp in tile_out(kind, j):
                cp.wait()
    for ch in (d2d, yA, *zA, *zB, yB, *fA[0], *fA[1], *fB[0], *fB[1], *gA, *gAy, *gB, gp):
        ch.drain()

    @pl.loop(0, N)
    def _(k):
        got(out.at[ds(row(k), BR), ds(col(k, 1 - c), H)], R["gp"](k))


def copy_kernel(*refs):
    ins, outs, (wide, slim, si, so) = refs[:4], refs[4:8], refs[8:]
    parts = []
    for a, b in zip(ins, outs):
        rows, cols = a.shape
        n = WR if cols == D else SR
        parts += [(a.at[pl.ds(r, n)], b.at[pl.ds(r, n)], wide if cols == D else slim) for r in range(0, rows, n)]

    def take(q):
        a, _, buf = parts[q]
        return pltpu.make_async_copy(a, buf.at[q % CR], si.at[q % CR])

    def give(q):
        _, b, buf = parts[q]
        return pltpu.make_async_copy(buf.at[q % CR], b, so.at[q % CR])

    for q in range(CR - CL):
        take(q).start()
    for q in range(len(parts)):
        take(q).wait()
        give(q).start()
        nxt = q + CR - CL
        if nxt < len(parts):
            if nxt >= CR:
                give(nxt - CR).wait()
            take(nxt).start()
    for q in range(len(parts) - CR, len(parts)):
        give(q).wait()


def solution(mesh):
    def step(x, dy, gate, up, w_gate, w_up, w_down):
        hbm = pl.BlockSpec(memory_space=pl.ANY)
        V, DMA = pltpu.VMEM, pltpu.SemaphoreType.DMA
        held = pl.pallas_call(
            kernel,
            name="mlp_bwd",
            out_shape=[
                jax.ShapeDtypeStruct((ROWS, D), BF16),
                jax.ShapeDtypeStruct((D, F), BF16),
                jax.ShapeDtypeStruct((D, F), BF16),
                jax.ShapeDtypeStruct((F, D), BF16),
            ],
            in_specs=[hbm] * 7,
            out_specs=[hbm] * 4,
            scratch_shapes=[
                V((F, D), BF16), V((D, F), BF16), V((D, F), BF16),
                V((ROWS, 2 * F), BF16), V((F, ROWS), BF16),
                V((4, ROWS, TW), BF16), V((BR, F), BF16), V((BR, F), BF16),
                V((DEPTH, BR, H), BF16), V((DR, BR, H), BF16),
                V((BR, H), F32), V((NS["A"], 256, H), F32), V((NS["B"], 512, H), F32),
                V((CNT["A"], 256, H), BF16), V((2, CNT["A"], 128, H), BF16),
                V((2, CNT["B"], 256, H), BF16), V((CNT["B"], 128, H), BF16),
                V((DEPTH, 256, H), BF16), V((2, DEPTH, 128, H), BF16), V((2, DEPTH, 256, H), BF16), V((DEPTH, 128, H), BF16),
                V((DEPTH, 128, H), BF16), V((DEPTH, 128, H), BF16),
                V((2, TW, 2 * F), BF16), V((2, F, TW), BF16),
                DMA((9,)), DMA((5, 2)), DMA((21, DEPTH)), DMA((17, N)),
                pltpu.SemaphoreType.REGULAR,
            ],
            compiler_params=pltpu.CompilerParams(has_side_effects=True, vmem_limit_bytes=67043328),
            cost_estimate=pl.CostEstimate(flops=77_000_000_000, bytes_accessed=100_000_000, transcendentals=0),
        )(x, dy, gate, up, w_gate, w_up, w_down)
        return pl.pallas_call(
            copy_kernel,
            name="results",
            out_shape=[jax.ShapeDtypeStruct(a.shape, a.dtype) for a in held],
            in_specs=[hbm] * 4,
            out_specs=[hbm] * 4,
            scratch_shapes=[V((CR, WR, D), BF16), V((CR, SR, F), BF16), DMA((CR,)), DMA((CR,))],
            compiler_params=pltpu.CompilerParams(vmem_limit_bytes=67043328),
        )(*held)

    tokens, columns, rows = P("dp", None), P(None, "tp"), P("tp", None)
    return jax.shard_map(
        step,
        mesh=mesh,
        in_specs=(tokens, tokens, P("dp", "tp"), P("dp", "tp"), columns, columns, rows),
        out_specs=(tokens, P("dp", "tp"), P("dp", "tp"), P(("dp", "tp"), None)),
        check_vma=False,
    )
```

```python
import functools

import jax
import jax.numpy as jnp
from jax import lax
from jax.experimental import pallas as pl
from jax.experimental.pallas import tpu as pltpu
from jax.sharding import PartitionSpec as P

F32, BF16 = jnp.float32, jnp.bfloat16
ROWS, D, F = 2048, 4096, 768
BR = 512
H = 256
NG = 2048 // H
N = (ROWS // BR) * NG
PAT = "AABAB"
PP = len(PAT)
CH = {r: [k for k in range(N) if PAT[k % PP] == r] for r in "AB"}
CNT = {r: len(CH[r]) for r in "AB"}
OFF = {"A": (0, 2, 7, 7, 10, 15, 17, 19, 31, 38), "B": (0, 2, 3, 5, 15, 20, 24, 26, 30, 38)}
ORDER = (10, 9, 2, 6, 4, 5, 8, 1, 3, 0, 7)
HS = (0, 5, 15, 20)
DW0 = 25
TW = 256
NW = D // TW
UP = PP - PP % 2
TT = max(-(-(N + OFF["A"][9]) // PP), DW0 // PP + 2 * NW // UP)


def turn(r, i, stage):
    return CH[r][i] + OFF[r][stage], ORDER.index(stage)


def slots(r):
    return next(n for n in range(1, CNT[r]) if all(turn(r, i + n, 1) > turn(r, i, 5) for i in range(CNT[r] - n)))


NS = {r: slots(r) for r in "AB"}
DEPTH = 4
DR = 8
WR, SR = 128, 512
CR, CL = 16, 8
NT = (((1,), (1,)), ((), ()))
TN = (((0,), (0,)), ((), ()))
NN = (((1,), (0,)), ((), ()))


def mm(a, b, dims):
    return lax.dot_general(a, b, dims, preferred_element_type=F32)


def ds(start, size):
    return pl.ds(pl.multiple_of(start, size), size)


class Chan:
    def __init__(self, n, cond, src, dst, send, recv=None, dev=None):
        self.n, self.cond, self.src, self.dst, self.send, self.recv, self.dev = n, cond, src, dst, send, recv, dev

    def desc(self, k, i):
        sem = self.send.at[lax.rem(i, DEPTH)]
        if self.dev is None:
            return pltpu.make_async_copy(self.src(k, i), self.dst(k, i), sem)
        return pltpu.make_async_remote_copy(
            self.src(k, i), self.dst(k, i), sem, self.recv(i), device_id=self.dev, device_id_type=pl.DeviceIdType.MESH
        )

    def wait(self, k, i):
        if self.dev is None:
            self.desc(k, i).wait()
        else:
            self.desc(k, i).wait_send()

    def ready(self, k, i):
        @pl.when(i >= DEPTH)
        def _():
            self.wait(k, i)

    def start(self, k, i):
        self.desc(k, i).start()

    def go(self, k, i):
        self.ready(k, i)
        self.start(k, i)

    def drain(self):
        def run():
            @pl.loop(self.n - DEPTH, self.n)
            def _(i):
                self.wait(0, i)

        if self.cond is None:
            run()
        else:
            pl.when(self.cond)(run)


def kernel(x, dy, gate, up, wg_h, wu_h, wd_h, out, dwg, dwu, dwd,
           wd, wg, wu, dgu, hT, xb, gb, ub, d2d_st, d2d_rv, tmp, accA, accB,
           yA_rv, zA_rv, zB_rv, yB_rv, yA_st, zA_st, zB_st, yB_st, fA_st, fB_st, o_gu, o_d,
           ld, tl, ss, rs, credit):
    tp = lax.axis_index("tp")
    y, z, c = tp // 8, lax.rem(tp // 2, 4), lax.rem(tp, 2)

    def dev(yy, zz, cc):
        return {"tp": yy * 8 + zz * 2 + cc}

    pair, ynb = dev(y, z, 1 - c), dev(1 - y, z, c)
    rt, lf = dev(y, jnp.minimum(z + 1, 3), c), dev(y, jnp.maximum(z - 1, 0), c)
    z0, z1, z2, z3 = z == 0, z == 1, z == 2, z == 3
    mid = jnp.logical_or(z1, z2)
    end = jnp.logical_or(z0, z3)
    nA, nB = CNT["A"], CNT["B"]

    def row(k):
        return (k // NG) * BR

    def col(k, cc):
        return cc * 2048 + lax.rem(k, NG) * H

    names_s = ["d2d", "yA", "zAR", "zAL", "zBR", "zBL", "yB", "fAl", "fAy", "fAz", "fBl", "fBy", "fBz",
               "gAR", "gAL", "gAyR", "gAyL", "gBy", "gBR", "gBL", "gp"]
    S = {n: ss.at[i] for i, n in enumerate(names_s)}
    names_r = ["yA", "zAR", "zAL", "zBR", "zBL", "yB", "gAR", "gAL", "gAyR", "gAyL", "gBy",
               "gBR0", "gBR1", "gBL0", "gBL1", "gp", "d2d"]
    R = {n: (lambda i, j=j: rs.at[j, i]) for j, n in enumerate(names_r)}

    def oA(k, yy, rl):
        return out.at[ds(row(k) + yy * 256 + rl * 128, 128), ds(col(k, c), H)]

    def oB(k, rl, yy):
        return out.at[ds(row(k) + rl * 256 + yy * 128, 128), ds(col(k, c), H)]

    def oB2(k, rl):
        return out.at[ds(row(k) + rl * 256, 256), ds(col(k, c), H)]

    def st(ref):
        return lambda k, i: ref.at[lax.rem(i, DEPTH)]

    def rv(ref):
        return lambda k, i: ref.at[i]

    d2d = Chan(N, None, st(d2d_st), lambda k, i: d2d_rv.at[lax.rem(i, DR)], S["d2d"],
               lambda i: R["d2d"](lax.rem(i, DR)), pair)
    yA = Chan(nA, None, st(yA_st), rv(yA_rv), S["yA"], R["yA"], ynb)
    zA = [Chan(nA, z < 3, st(zA_st.at[0]), rv(zA_rv.at[0]), S["zAR"], R["zAR"], rt),
          Chan(nA, z > 0, st(zA_st.at[1]), rv(zA_rv.at[1]), S["zAL"], R["zAL"], lf)]
    zB = [Chan(nB, z < 3, st(zB_st.at[0]), rv(zB_rv.at[0]), S["zBR"], R["zBR"], rt),
          Chan(nB, z > 0, st(zB_st.at[1]), rv(zB_rv.at[1]), S["zBL"], R["zBL"], lf)]
    yB = Chan(nB, end, st(yB_st), rv(yB_rv), S["yB"], R["yB"], ynb)
    fA, fB, gA, gAy, gB, loc = [], [], [], [], [], []
    for rl, (fin, back, recvs) in enumerate(((z3, lf, ("gAR", "gAyR")), (z0, rt, ("gAL", "gAyL")))):
        o = lambda k, i, rl=rl: oA(k, y, rl)
        fA.append([Chan(nA, fin, st(fA_st), o, S["fAy"], R[recvs[1]], ynb),
                   Chan(nA, fin, st(fA_st), o, S["fAz"], R[recvs[0]], back)])
        gA.append(Chan(nA, mid, o, o, S["gAR" if rl == 0 else "gAL"], R[recvs[0]], back))
        nf = (z < 3) if rl == 0 else (z > 0)
        gAy.append(Chan(nA, nf, o, o, S["gAyR" if rl == 0 else "gAyL"], R[recvs[1]], ynb))
        ob = lambda k, i, rl=rl: oB(k, rl, y)
        ob_other = lambda k, i, rl=rl: oB(k, rl, 1 - y)
        nm = "gBR" if rl == 0 else "gBL"
        by_y = lambda me, nm=nm: (lambda i: rs.at[names_r.index(nm + "0") + me, i])
        fB.append([Chan(nB, fin, st(fB_st), ob, S["fBy"], R["gBy"], ynb),
                   Chan(nB, fin, st(fB_st), ob, S["fBz"], by_y(y), back),
                   Chan(nB, fin, ob_other, ob_other, S["gBy"], by_y(1 - y), back)])
        ob2 = lambda k, i, rl=rl: oB2(k, rl)
        gB.append(Chan(nB, mid, ob2, ob2, S[nm], R[nm + "0"], back))
        loc.append((Chan(nA, fin, st(fA_st), o, S["fAl"]), Chan(nB, fin, st(fB_st), ob, S["fBl"])))
    whole = lambda k, i: out.at[ds(row(k), BR), ds(col(k, c), H)]
    gp = Chan(N, None, whole, whole, S["gp"], R["gp"], pair)

    def got(dst, sem):
        pltpu.make_async_copy(dst, dst, sem).wait()

    def dy_block(b):
        r = ds(b * BR, BR)
        cps = [pltpu.make_async_copy(dy.at[r, pl.ds(p * 256, 256)], xb.at[p // 4, pl.ds((p % 4) * 512, 512)], ld.at[3])
               for p in range(16)]
        return cps + [pltpu.make_async_copy(gate.at[r], gb, ld.at[4]), pltpu.make_async_copy(up.at[r], ub, ld.at[5])]

    barrier = pltpu.get_barrier_semaphore()
    for cond, d in ((None, pair), (None, ynb), (z < 3, rt), (z > 0, lf)):
        def hello(d=d):
            pl.semaphore_signal(barrier, 1, device_id=d, device_id_type=pl.DeviceIdType.MESH)

        if cond is None:
            hello()
        else:
            pl.when(cond)(hello)

    def wd_part(n):
        return pltpu.make_async_copy(wd_h.at[ds(n * 256, 256)], wd.at[ds(n * 256, 256)], ld.at[6 + n])

    wd_part(0).start()
    for cp in dy_block(0):
        cp.start()
    wd_part(1).start()
    wd_part(2).start()
    pltpu.make_async_copy(wg_h, wg, ld.at[1]).start()
    pltpu.make_async_copy(wu_h, wu, ld.at[2]).start()

    pl.semaphore_wait(barrier, jnp.where(end, 3, 4))

    def tile(kind, j):
        s = lax.rem(j, 2)
        return pltpu.make_async_copy((x, dy)[kind].at[:, ds(j * TW, TW)], xb.at[2 * kind + s], tl.at[kind, s])

    def tile_out(kind, j):
        s = lax.rem(j, 2)
        if kind == 0:
            return [pltpu.make_async_copy(o_gu.at[s, :, pl.ds(0, F)], dwg.at[ds(j * TW, TW)], tl.at[2, s]),
                    pltpu.make_async_copy(o_gu.at[s, :, pl.ds(F, F)], dwu.at[ds(j * TW, TW)], tl.at[3, s])]
        return [pltpu.make_async_copy(o_d.at[s], dwd.at[:, ds(j * TW, TW)], tl.at[4, s])]

    def hidden_block(b):
        got(xb, ld.at[3])
        got(gb, ld.at[4])
        got(ub, ld.at[5])
        r = ds(b * BR, BR)

        @pl.loop(0, F // 256)
        def _(n):
            pl.when(b == 0)(lambda: wd_part(n).wait())
            f = ds(n * 256, 256)
            dh = sum(mm(xb[p // 4, pl.ds((p % 4) * 512, 512), :], wd[f, pl.ds(p * 256, 256)], NT) for p in range(16))
            g, u = gb[:, f].astype(F32), ub[:, f].astype(F32)
            sig = jax.nn.sigmoid(g)
            silu = g * sig
            hT[f, r] = (silu * u).T.astype(BF16)
            dgu[r, f] = (dh * u * (sig + silu * (1.0 - sig))).astype(BF16)
            dgu[r, ds(F + n * 256, 256)] = (dh * silu).astype(BF16)

        @pl.when(b + 1 < ROWS // BR)
        def _():
            for cp in dy_block(b + 1):
                cp.start()

        @pl.when(b + 1 == ROWS // BR)
        def _():
            tile(0, 0).start()
            tile(1, 0).start()

    def term(k, cols):
        r = ds(row(k), BR)
        return mm(dgu[r, pl.ds(0, F)], wg[cols, :], NT) + mm(dgu[r, pl.ds(F, F)], wu[cols, :], NT)

    def a0(k, i, cls):
        @pl.when(k == 0)
        def _():
            pltpu.make_async_copy(wg_h, wg, ld.at[1]).wait()
            pltpu.make_async_copy(wu_h, wu, ld.at[2]).wait()

        d2d.ready(k, k)
        d2d_st[lax.rem(k, DEPTH)] = term(k, ds(col(k, 1 - c), H)).astype(BF16)

        @pl.when(k >= DR)
        def _():
            pl.semaphore_wait(credit, 1)

        d2d.start(k, k)

    def a1(k, i, cls):
        s, q, s8 = lax.rem(i, NS[cls]), lax.rem(i, DEPTH), lax.rem(k, DR)
        got(d2d_rv.at[s8], R["d2d"](s8))
        if cls == "A":
            yA.ready(k, i)
            tmp[...] = term(k, ds(col(k, c), H)) + d2d_rv[s8].astype(F32)
            yA_st[q] = tmp[ds((1 - y) * 256, 256), :].astype(BF16)
            yA.start(k, i)
            accA[s] = tmp[ds(y * 256, 256), :]
        else:
            accB[s] = term(k, ds(col(k, c), H)) + d2d_rv[s8].astype(F32)
            for rl, first in ((0, z0), (1, z3)):
                @pl.when(first)
                def _():
                    zB[rl].ready(k, i)
                    zB_st[rl, q] = accB[s, pl.ds(rl * 256, 256), :].astype(BF16)
                    zB[rl].start(k, i)

        @pl.when(k < N - DR)
        def _():
            pl.semaphore_signal(credit, 1, device_id=pair, device_id_type=pl.DeviceIdType.MESH)

    def passA(k, i, rl):
        s, q = lax.rem(i, NS["A"]), lax.rem(i, DEPTH)
        got(zA_rv.at[rl, i], R["zAR" if rl == 0 else "zAL"](i))
        zA[rl].ready(k, i)
        zA_st[rl, q] = (accA[s, pl.ds(rl * 128, 128), :] + zA_rv[rl, i].astype(F32)).astype(BF16)
        zA[rl].start(k, i)

    def passB(k, i, rl):
        s, q = lax.rem(i, NS["B"]), lax.rem(i, DEPTH)
        got(zB_rv.at[rl, i], R["zBR" if rl == 0 else "zBL"](i))
        zB[rl].ready(k, i)
        zB_st[rl, q] = (accB[s, pl.ds(rl * 256, 256), :] + zB_rv[rl, i].astype(F32)).astype(BF16)
        zB[rl].start(k, i)

    def a2(k, i, cls):
        s, q = lax.rem(i, NS[cls]), lax.rem(i, DEPTH)
        if cls == "B":
            pl.when(z1)(lambda: passB(k, i, 0))
            pl.when(z2)(lambda: passB(k, i, 1))
            return
        got(yA_rv.at[i], R["yA"](i))
        accA[s] = accA[s] + yA_rv[i].astype(F32)
        for rl, first in ((0, z0), (1, z3)):
            @pl.when(first)
            def _():
                zA[rl].ready(k, i)
                zA_st[rl, q] = accA[s, pl.ds(rl * 128, 128), :].astype(BF16)
                zA[rl].start(k, i)

    def a3(k, i, cls):
        if cls == "B":
            pl.when(z2)(lambda: passB(k, i, 0))
            pl.when(z1)(lambda: passB(k, i, 1))
        else:
            pl.when(z1)(lambda: passA(k, i, 0))
            pl.when(z2)(lambda: passA(k, i, 1))

    def a4(k, i, cls):
        s, q = lax.rem(i, NS[cls]), lax.rem(i, DEPTH)
        if cls == "A":
            pl.when(z2)(lambda: passA(k, i, 0))
            pl.when(z1)(lambda: passA(k, i, 1))
            return
        for rl, fin in ((0, z3), (1, z0)):
            @pl.when(fin)
            def _():
                got(zB_rv.at[rl, i], R["zBR" if rl == 0 else "zBL"](i))
                yB.ready(k, i)
                r = pl.ds(rl * 256, 256)
                accB[s, r, :] = accB[s, r, :] + zB_rv[rl, i].astype(F32)
                yB_st[q] = accB[s, ds(rl * 256 + (1 - y) * 128, 128), :].astype(BF16)
                yB.start(k, i)

    def a5(k, i, cls):
        s, q = lax.rem(i, NS[cls]), lax.rem(i, DEPTH)
        for rl, fin in ((0, z3), (1, z0)):
            @pl.when(fin)
            def _():
                if cls == "B":
                    got(yB_rv.at[i], R["yB"](i))
                    for ch in fB[rl][:2]:
                        ch.ready(k, i)
                    fB_st[q] = (accB[s, ds(rl * 256 + y * 128, 128), :] + yB_rv[i].astype(F32)).astype(BF16)
                    for ch in (*fB[rl][:2], loc[rl][1]):
                        ch.start(k, i)
                else:
                    got(zA_rv.at[rl, i], R["zAR" if rl == 0 else "zAL"](i))
                    for ch in fA[rl]:
                        ch.ready(k, i)
                    fA_st[q] = (accA[s, pl.ds(rl * 128, 128), :] + zA_rv[rl, i].astype(F32)).astype(BF16)
                    for ch in (*fA[rl], loc[rl][0]):
                        ch.start(k, i)

    def fwdA(k, i, rl, z_too):
        got(oA(k, y, rl), R["gAR" if rl == 0 else "gAL"](i))
        if z_too:
            gA[rl].go(k, i)
        gAy[rl].go(k, i)

    def a6(k, i, cls):
        if cls == "A":
            pl.when(z2)(lambda: fwdA(k, i, 0, True))
            pl.when(z1)(lambda: fwdA(k, i, 1, True))
            return
        for rl, fin in ((0, z3), (1, z0)):
            @pl.when(fin)
            def _():
                got(oB(k, rl, 1 - y), R["gBy"](i))
                fB[rl][2].go(k, i)

    def a7(k, i, cls):
        if cls == "A":
            pl.when(z1)(lambda: fwdA(k, i, 0, True))
            pl.when(z2)(lambda: fwdA(k, i, 1, True))
            return
        for rl, m in ((0, z2), (1, z1)):
            @pl.when(m)
            def _():
                nm = "gBR" if rl == 0 else "gBL"
                for yy in range(2):
                    got(oB(k, rl, yy), R[nm + str(yy)](i))
                gB[rl].go(k, i)

    def a8(k, i, cls):
        if cls == "A":
            pl.when(z0)(lambda: fwdA(k, i, 0, False))
            pl.when(z3)(lambda: fwdA(k, i, 1, False))
            return
        for rl, m in ((0, z1), (1, z2)):
            @pl.when(m)
            def _():
                got(oB2(k, rl), R["gBR0" if rl == 0 else "gBL0"](i))
                gB[rl].go(k, i)

    def a9(k, i, cls):
        for rl, m in enumerate((z0, z3)):
            if cls == "B":
                @pl.when(m)
                def _():
                    got(oB2(k, rl), R["gBR0" if rl == 0 else "gBL0"](i))
            else:
                got(oA(k, 1 - y, rl), R["gAyR" if rl == 0 else "gAyL"](i))
        gp.go(k, k)

    def weights(kind, j):
        tile(kind, j).wait()

        @pl.when(j + 1 < NW)
        def _():
            tile(kind, j + 1).start()

        @pl.when(j >= 2)
        def _():
            for cp in tile_out(kind, j - 2):
                cp.wait()

        s = lax.rem(j, 2)
        if kind == 0:
            o_gu[s] = mm(xb[s], dgu[...], TN).astype(BF16)
        else:
            o_d[s] = mm(hT[...], xb[2 + s], NN).astype(BF16)
        for cp in tile_out(kind, j):
            cp.start()

    stages = (a0, a1, a2, a3, a4, a5, a6, a7, a8, a9)

    def settle(k, i, cls):
        for rl, fin in ((0, z3), (1, z0)):
            pl.when(fin)(lambda: loc[rl]["AB".index(cls)].wait(k, i))

    @pl.loop(0, TT)
    def _(tt):
        for par in range(PP):
            t = tt * PP + par

            def chunk(cls, stage, run):
                ph = (par - OFF[cls][stage]) % PP
                if PAT[ph] != cls:
                    return
                rnd = tt + (par - OFF[cls][stage] - ph) // PP
                k, i = rnd * PP + ph, rnd * PAT.count(cls) + PAT[:ph].count(cls)

                @pl.when(jnp.logical_and(k >= 0, k < N))
                def _():
                    run(k, i, cls)

            if par == 0:
                b = sum((t >= s).astype(jnp.int32) for s in HS[1:])
                pl.when(functools.reduce(jnp.logical_or, [t == s for s in HS]))(lambda: hidden_block(b))
            for stage in ORDER:
                if stage == 0:
                    pl.when(t < N)(lambda: a0(t, t, None))
                elif stage == 10:
                    j = (tt - DW0 // PP) * (UP // 2) + par // 2

                    if par < UP:
                        @pl.when(jnp.logical_and(tt >= DW0 // PP, j < NW))
                        def _():
                            weights(par % 2, j)
                else:
                    for cls in "AB":
                        chunk(cls, stage, stages[stage])
            for cls in "AB":
                chunk(cls, 5, settle)

    for kind in range(2):
        for j in (NW - 2, NW - 1):
            for cp in tile_out(kind, j):
                cp.wait()
    for ch in (d2d, yA, *zA, *zB, yB, *fA[0], *fA[1], *fB[0], *fB[1], *gA, *gAy, *gB, gp):
        ch.drain()

    @pl.loop(0, N)
    def _(k):
        got(out.at[ds(row(k), BR), ds(col(k, 1 - c), H)], R["gp"](k))


def copy_kernel(*refs):
    ins, outs, (wide, slim, si, so) = refs[:4], refs[4:8], refs[8:]
    parts = []
    for a, b in zip(ins, outs):
        rows, cols = a.shape
        n = WR if cols == D else SR
        parts += [(a.at[pl.ds(r, n)], b.at[pl.ds(r, n)], wide if cols == D else slim) for r in range(0, rows, n)]

    def take(q):
        a, _, buf = parts[q]
        return pltpu.make_async_copy(a, buf.at[q % CR], si.at[q % CR])

    def give(q):
        _, b, buf = parts[q]
        return pltpu.make_async_copy(buf.at[q % CR], b, so.at[q % CR])

    for q in range(CR - CL):
        take(q).start()
    for q in range(len(parts)):
        take(q).wait()
        give(q).start()
        nxt = q + CR - CL
        if nxt < len(parts):
            if nxt >= CR:
                give(nxt - CR).wait()
            take(nxt).start()
    for q in range(len(parts) - CR, len(parts)):
        give(q).wait()


def solution(mesh):
    def step(x, dy, gate, up, w_gate, w_up, w_down):
        hbm = pl.BlockSpec(memory_space=pl.ANY)
        V, DMA = pltpu.VMEM, pltpu.SemaphoreType.DMA
        held = pl.pallas_call(
            kernel,
            name="mlp_bwd",
            out_shape=[
                jax.ShapeDtypeStruct((ROWS, D), BF16),
                jax.ShapeDtypeStruct((D, F), BF16),
                jax.ShapeDtypeStruct((D, F), BF16),
                jax.ShapeDtypeStruct((F, D), BF16),
            ],
            in_specs=[hbm] * 7,
            out_specs=[hbm] * 4,
            scratch_shapes=[
                V((F, D), BF16), V((D, F), BF16), V((D, F), BF16),
                V((ROWS, 2 * F), BF16), V((F, ROWS), BF16),
                V((4, ROWS, TW), BF16), V((BR, F), BF16), V((BR, F), BF16),
                V((DEPTH, BR, H), BF16), V((DR, BR, H), BF16),
                V((BR, H), F32), V((NS["A"], 256, H), F32), V((NS["B"], 512, H), F32),
                V((CNT["A"], 256, H), BF16), V((2, CNT["A"], 128, H), BF16),
                V((2, CNT["B"], 256, H), BF16), V((CNT["B"], 128, H), BF16),
                V((DEPTH, 256, H), BF16), V((2, DEPTH, 128, H), BF16), V((2, DEPTH, 256, H), BF16), V((DEPTH, 128, H), BF16),
                V((DEPTH, 128, H), BF16), V((DEPTH, 128, H), BF16),
                V((2, TW, 2 * F), BF16), V((2, F, TW), BF16),
                DMA((9,)), DMA((5, 2)), DMA((21, DEPTH)), DMA((17, N)),
                pltpu.SemaphoreType.REGULAR,
            ],
            compiler_params=pltpu.CompilerParams(collective_id=0, has_side_effects=True, vmem_limit_bytes=67043328),
            cost_estimate=pl.CostEstimate(flops=77_000_000_000, bytes_accessed=100_000_000, transcendentals=0),
        )(x, dy, gate, up, w_gate, w_up, w_down)
        return pl.pallas_call(
            copy_kernel,
            name="results",
            out_shape=[jax.ShapeDtypeStruct(a.shape, a.dtype) for a in held],
            in_specs=[hbm] * 4,
            out_specs=[hbm] * 4,
            scratch_shapes=[V((CR, WR, D), BF16), V((CR, SR, F), BF16), DMA((CR,)), DMA((CR,))],
            compiler_params=pltpu.CompilerParams(vmem_limit_bytes=67043328),
        )(*held)

    tokens, columns, rows = P("dp", None), P(None, "tp"), P("tp", None)
    return jax.shard_map(
        step,
        mesh=mesh,
        in_specs=(tokens, tokens, P("dp", "tp"), P("dp", "tp"), columns, columns, rows),
        out_specs=(tokens, P("dp", "tp"), P("dp", "tp"), P(("dp", "tp"), None)),
        check_vma=False,
    )
```
